32 devices in a mesh: pipe: 4 (over y, core), tensor: 8 (over z, x).
Axes of the slice: x: 2, y: 2, z: 4, core: 2. Of those that a mesh axis runs over, the one named last changes fastest.
Arguments:
- patches: bfloat16 [16384, 1280], P(('pipe', 'tensor')), may hold values from -6 to 6
- attn_gain: float32 [1280], replicated, may hold values from 0.25 to 1.75
- w_qkv: bfloat16 [1280, 3840], P('tensor', 'pipe'), may hold values from -0.1118034 to 0.1118034
- w_out: bfloat16 [1280, 1280], P('tensor', 'pipe'), may hold values from -0.15625 to 0.15625
- merge_gain: float32 [1280], replicated, may hold values from 0.25 to 1.75
- window_ids: int32 [16384], P(('pipe', 'tensor')), may hold values from 0 to 127, as said below
- image_patches: int32 [128], P(('pipe', 'tensor')), may hold values from 0 to 512, as said below
- image_sample: int32 [128], P(('pipe', 'tensor')), may hold values from 0 to 7
Outputs:
- vision_seq: bfloat16 [4, 128, 8, 5120], P('pipe', None, 'tensor')
The draws below stay inside these ranges and needn't reach their ends.
Inputs may be any that keep to these rules, and one draw needn't show every extreme that they name: `window_ids`: Non-decreasing within each bundle and equal over each 4 consecutive slots; every window lies within one aligned block of 64 slots of a bundle. `image_patches`: multiples of 128; the images of one bundle take at most 512 slots and at least half of them, and in every micro-batch some bundle is full.
All inputs are finite; a program needn't handle non-finite values.
Results may differ from the reference program's by a relative error of at most 0.0053.
Values may be sent and summed in bfloat16 or wider, within the bound.
A program may use at most 64 MiB of HBM per device.

```python
import math
import jax
import jax.numpy as jnp
from jax import lax

D = 1280
HEADS = 16
WINDOW = 64
IMG_DEV = 4
P_DEV = 512
SAMPLES = 8
GROUP = 8
MICRO = 4
BUNDLES = 32
PATCHES = 16384
IMAGES = 128


def draw_window_ids(key, part):
    group_slots = P_DEV // 4
    coin_flip = jax.random.randint(jax.random.fold_in(key, 11), (BUNDLES, group_slots), 0, 6)
    slot_index = jnp.arange(group_slots, dtype=jnp.int32)
    forced = (slot_index % (WINDOW // 4) == 0)[None, :]
    finest = (jnp.arange(BUNDLES, dtype=jnp.int32) == 0)[:, None]
    window_starts = jnp.where(forced | finest | (coin_flip == 0), 1, 0).astype(jnp.int32)
    window_index = jnp.cumsum(window_starts, axis=1) - 1
    return jnp.repeat(window_index, 4, axis=1).reshape(BUNDLES * P_DEV).astype(jnp.int32)


def draw_image_patches(key, part):
    unit_count = P_DEV // 128
    lowest = (unit_count + 1) // 2
    totals = jax.random.randint(jax.random.fold_in(key, 21), (BUNDLES,), lowest, unit_count + 1)
    full_member = jax.random.randint(jax.random.fold_in(key, 22), (MICRO,), 0, GROUP)
    bundle_index = jnp.arange(BUNDLES, dtype=jnp.int32)
    totals = jnp.where((bundle_index % GROUP == full_member[bundle_index // GROUP]) | (bundle_index == 0), unit_count, totals)
    slot_choice = jax.random.randint(jax.random.fold_in(key, 23), (BUNDLES, unit_count), 0, IMG_DEV)
    single_slot = jax.random.randint(jax.random.fold_in(key, 24), (), 0, IMG_DEV)
    slot_choice = jnp.where((bundle_index == 0)[:, None], single_slot, slot_choice)
    active = jnp.arange(unit_count, dtype=jnp.int32)[None, :] < totals[:, None]
    matches = (slot_choice[:, :, None] == jnp.arange(IMG_DEV, dtype=jnp.int32)[None, None, :]) & active[:, :, None]
    counts = jnp.sum(matches.astype(jnp.int32), axis=1) * 128
    return counts.reshape(BUNDLES * IMG_DEV).astype(jnp.int32)


def draw_patches(key, part):
    rows = jax.random.normal(jax.random.fold_in(key, 45), (PATCHES, D), jnp.float32)
    return jnp.clip(rows, -6.0, 6.0).astype(jnp.bfloat16)


def draw_w_qkv(key, part):
    unit = 1.0 / math.sqrt(D)
    base = jax.random.normal(jax.random.fold_in(key, 52), (D, 3 * D), jnp.float32)
    return (jnp.clip(base, -3.98, 3.98) * unit).astype(jnp.bfloat16)


def touch_ends(array, key, low, largest):
    extent = array.shape
    index_at = [jax.random.randint(jax.random.fold_in(key, axis), (), 0, extent[axis]) for axis in range(len(extent))]
    array = array.at[tuple(index_at)].set(low)
    longest = extent.index(max(extent))
    index_at[longest] = (index_at[longest] + 1) % extent[longest]
    return array.at[tuple(index_at)].set(largest)


def level_of(stream_key, shape, split, smallest, largest):
    def one(axis_at, parts):
        steps = jax.random.uniform(jax.random.fold_in(jax.random.fold_in(stream_key, 6), axis_at), (parts,), jnp.float32, smallest / len(split), largest / len(split))
        return jnp.repeat(jnp.exp(steps), shape[axis_at] // parts).reshape((-1,) + (1,) * (len(shape) - axis_at - 1))

    level = one(*split[0])
    for cut in split[1:]:
        level = level * one(*cut)
    return level


def bell_draw(rng, extent, scale, limit, split=(), kind=jnp.bfloat16):
    values = scale * jax.random.normal(rng, extent, jnp.float32)
    if split:
        values = values * level_of(rng, extent, split, -0.22, 0.18)
    return jnp.clip(values, -limit, limit).astype(kind)


def setup_inputs(seed: int = 0) -> dict:
    seeds = jax.random.split(jax.random.key(seed), 9)
    return {
        "patches": draw_patches(jax.random.fold_in(seeds[8], 71), 0),
        "attn_gain": jnp.clip(1.0 + 0.15 * jax.random.normal(seeds[1], (D,), jnp.float32), 0.25, 1.75),
        "w_qkv": draw_w_qkv(jax.random.fold_in(seeds[8], 71), 0),
        "w_out": bell_draw(seeds[3], (D, D), D ** -0.5, 0.15625, ((0, 8), (1, 4))),
        "merge_gain": jnp.clip(1.0 + 0.15 * jax.random.normal(seeds[4], (D,), jnp.float32), 0.25, 1.75),
        "window_ids": draw_window_ids(jax.random.fold_in(seeds[8], 71), 0),
        "image_patches": draw_image_patches(jax.random.fold_in(seeds[8], 71), 0),
        "image_sample": touch_ends(jax.random.randint(seeds[7], (IMAGES,), 0, SAMPLES), jax.random.fold_in(seeds[7], 1), 0, SAMPLES - 1).astype(jnp.int32),
    }


epsilon = 1e-06

def normalize(values, gain_row):
    return values * lax.rsqrt(lax.optimization_barrier(jnp.mean(values * values, axis=-1, keepdims=True)) + epsilon) * gain_row

def encode_bundle(patch_rows, window_row, live_row, attn_gain, w_qkv, w_out, merge_gain):
    residual = patch_rows.astype(jnp.float32)
    normed = normalize(residual, attn_gain).astype(jnp.bfloat16)
    qkv = jnp.dot(normed, w_qkv, preferred_element_type=jnp.float32).astype(jnp.bfloat16)
    head_width = D // HEADS
    tile_count = P_DEV // WINDOW

    def split_heads(block):
        return block.reshape(tile_count, WINDOW, HEADS, head_width).astype(jnp.float32)
    queries = split_heads(qkv[:, :D])
    keys_tile = split_heads(qkv[:, D:2 * D])
    values_tile = split_heads(qkv[:, 2 * D:])
    scores = jnp.einsum('tqhd,tkhd->thqk', queries, keys_tile) * (1.0 / math.sqrt(head_width))
    window_tile = window_row.reshape(tile_count, WINDOW)
    live_tile = live_row.reshape(tile_count, WINDOW)
    allowed = (window_tile[:, :, None] == window_tile[:, None, :]) & live_tile[:, None, :]
    scores = jnp.where(allowed[:, None, :, :], scores, -1e+30)
    row_max = lax.optimization_barrier(jnp.max(scores, axis=-1, keepdims=True))
    exponent = jnp.exp(scores - row_max)
    weights = (exponent / lax.optimization_barrier(jnp.sum(exponent, axis=-1, keepdims=True))).astype(jnp.bfloat16)
    context = jnp.einsum('thqk,tkhd->tqhd', weights.astype(jnp.float32), values_tile).reshape(P_DEV, D)
    context = jnp.where(live_row[:, None], context, 0.0).astype(jnp.bfloat16)
    hidden = residual + jnp.dot(context, w_out, preferred_element_type=jnp.float32)
    merged = normalize(hidden, merge_gain).astype(jnp.bfloat16)
    return merged.reshape(P_DEV // 4, 4 * D)

def image_starts(merged_count, samples):
    image_order = jnp.arange(merged_count.shape[0], dtype=jnp.int32)
    ahead = (samples[None, :] < samples[:, None]) | (samples[None, :] == samples[:, None]) & (image_order[None, :] < image_order[:, None])
    return lax.optimization_barrier(jnp.sum(jnp.where(ahead, merged_count[None, :], 0), axis=1)).astype(jnp.int32)

def token_positions(starts, merged_count):
    token_count = P_DEV // 4
    offsets = (jnp.cumsum(merged_count) - merged_count).astype(jnp.int32)
    token_index = jnp.arange(token_count, dtype=jnp.int32)
    inside = (token_index[None, :] >= offsets[:, None]) & (token_index[None, :] < (offsets + merged_count)[:, None])
    position = lax.optimization_barrier(jnp.sum(jnp.where(inside, starts[:, None] + token_index[None, :] - offsets[:, None], 0), axis=0))
    return jnp.where(jnp.any(inside, axis=0), position, -1).astype(jnp.int32)

def reference(patches, attn_gain, w_qkv, w_out, merge_gain, window_ids, image_patches, image_sample):
    token_count = P_DEV // 4
    grouped = (patches.reshape(MICRO, GROUP, P_DEV, D), window_ids.reshape(MICRO, GROUP, P_DEV), image_patches.reshape(MICRO, GROUP, IMG_DEV), image_sample.reshape(MICRO, GROUP, IMG_DEV))

    def one_group(members):
        group_patches, group_windows, group_counts, group_samples = members
        live = jnp.arange(P_DEV, dtype=jnp.int32)[None, :] < lax.optimization_barrier(jnp.sum(group_counts, axis=1))[:, None]

        def encode_member(member):
            return encode_bundle(member[0], member[1], member[2], attn_gain, w_qkv, w_out, merge_gain)
        tokens = lax.map(encode_member, (group_patches, group_windows, live))
        merged_count = (group_counts // 4).astype(jnp.int32)
        starts = image_starts(merged_count.reshape(-1), group_samples.reshape(-1)).reshape(GROUP, IMG_DEV)
        positions = jax.vmap(token_positions)(starts, merged_count)
        positions = jnp.where(positions < 0, GROUP * token_count, positions).astype(jnp.int32)
        sequence = jnp.zeros((GROUP * token_count, 4 * D), jnp.bfloat16)
        sequence = sequence.at[positions.reshape(-1)].set(tokens.reshape(-1, 4 * D), mode='drop')
        return sequence.reshape(token_count, GROUP, 4 * D)
    return lax.map(one_group, grouped)
```

```python
import functools
import math

import jax
import jax.numpy as jnp
from jax import lax
from jax.experimental import pallas as pl
from jax.experimental.pallas import tpu as pltpu
from jax.sharding import PartitionSpec as P

HEADS = 16
WINDOW = 64
SAMPLES = 8


epsilon = 1e-06


def normalize(values, gain_row):
    return (
        values * lax.rsqrt(jnp.mean(values * values, axis=-1, keepdims=True) + epsilon) * gain_row
    )


def token_positions(starts, merged_count, token_count):
    offsets = jnp.cumsum(merged_count) - merged_count
    token_index = jnp.arange(token_count, dtype=jnp.int32)
    inside = (token_index[None, :] >= offsets[:, None]) & (
        token_index[None, :] < (offsets + merged_count)[:, None]
    )
    position = jnp.sum(
        jnp.where(inside, starts[:, None] + token_index[None, :] - offsets[:, None], 0), axis=0
    )
    return jnp.where(jnp.any(inside, axis=0), position, -1)


def body(patches, attn_gain, w_qkv, w_out, merge_gain, window_ids, image_patches, image_sample):
    patch_count, feature_width = patches.shape
    token_count = patch_count // 4
    group_size = lax.axis_size("tensor")
    own_index = lax.axis_index("tensor")
    residual = patches.astype(jnp.float32)
    normed = normalize(residual, attn_gain).astype(jnp.bfloat16)
    qkv_rows = lax.all_gather(w_qkv, "tensor", axis=0, tiled=True)
    qkv = jnp.dot(
        normed,
        lax.all_gather(qkv_rows, "pipe", axis=1, tiled=True),
        preferred_element_type=jnp.float32,
    ).astype(jnp.bfloat16)
    head_width = feature_width // HEADS
    tile_count = patch_count // WINDOW

    def split_heads(block):
        return block.reshape(tile_count, WINDOW, HEADS, head_width)

    queries = split_heads(qkv[:, :feature_width])
    keys_tile = split_heads(qkv[:, feature_width : 2 * feature_width])
    values_tile = split_heads(qkv[:, 2 * feature_width :])
    scores = jnp.einsum(
        "tqhd,tkhd->thqk", queries, keys_tile, preferred_element_type=jnp.float32
    ) * (1.0 / math.sqrt(head_width))
    live_row = jnp.arange(patch_count, dtype=jnp.int32) < jnp.sum(image_patches)
    window_tile = window_ids.reshape(tile_count, WINDOW)
    live_tile = live_row.reshape(tile_count, WINDOW)
    allowed = (window_tile[:, :, None] == window_tile[:, None, :]) & live_tile[:, None, :]
    scores = jnp.where(allowed[:, None, :, :], scores, -1e30)
    row_max = jnp.max(scores, axis=-1, keepdims=True)
    exponent = jnp.exp(scores - row_max)
    weights = (exponent / jnp.sum(exponent, axis=-1, keepdims=True)).astype(jnp.bfloat16)
    context = jnp.einsum(
        "thqk,tkhd->tqhd", weights, values_tile, preferred_element_type=jnp.float32
    ).reshape(patch_count, feature_width)
    context = jnp.where(live_row[:, None], context, 0.0).astype(jnp.bfloat16)
    proj_rows = lax.all_gather(w_out, "tensor", axis=0, tiled=True)
    attended = jnp.dot(
        context,
        lax.all_gather(proj_rows, "pipe", axis=1, tiled=True),
        preferred_element_type=jnp.float32,
    )
    hidden = residual + attended
    merged = (
        normalize(hidden, merge_gain).astype(jnp.bfloat16).reshape(token_count, 4 * feature_width)
    )
    outgoing = merged.reshape(token_count // group_size, group_size, 4 * feature_width)
    merged_count = image_patches // 4
    sample_hot = image_sample[:, None] == jnp.arange(SAMPLES, dtype=jnp.int32)[None, :]
    sample_tally = jnp.sum(jnp.where(sample_hot, merged_count[:, None], 0), axis=0)
    all_tallies = lax.all_gather(sample_tally[None, :], "tensor", axis=0, tiled=True)
    source_ranks = jnp.arange(group_size, dtype=jnp.int32)
    before = jnp.sum(jnp.where((source_ranks < own_index)[:, None], all_tallies, 0), axis=0)
    totals = jnp.sum(all_tallies, axis=0)
    sample_index = jnp.arange(SAMPLES, dtype=jnp.int32)
    sample_base = jnp.sum(
        jnp.where(sample_index[None, :] < sample_index[:, None], totals[None, :], 0), axis=1
    )
    image_order = jnp.arange(image_sample.shape[0], dtype=jnp.int32)
    same_before = (image_sample[None, :] == image_sample[:, None]) & (
        image_order[None, :] < image_order[:, None]
    )
    earlier = jnp.sum(jnp.where(same_before, merged_count[None, :], 0), axis=1)
    starts = jnp.sum(jnp.where(sample_hot, (sample_base + before)[None, :], 0), axis=1) + earlier
    position = token_positions(starts, merged_count, token_count)
    outgoing_position = position.reshape(token_count // group_size, group_size)
    received, received_position = (
        lax.all_to_all(outgoing, "tensor", split_axis=1, concat_axis=0, tiled=True),
        lax.all_to_all(outgoing_position, "tensor", split_axis=1, concat_axis=0, tiled=True),
    )
    dest_rows = received_position.reshape(token_count) // group_size
    placement = (jnp.arange(token_count, dtype=jnp.int32)[:, None] == dest_rows[None, :]).astype(
        jnp.bfloat16
    )
    placed = jnp.dot(
        placement,
        received.reshape(token_count, 4 * feature_width),
        preferred_element_type=jnp.float32,
    )
    return placed.astype(jnp.bfloat16).reshape(1, token_count, 1, 4 * feature_width)


CORES = 2
CHIPS_X = 2
MESH = pl.DeviceIdType.MESH


def kernel(
    lines, group, x_ref, gain_ref, wq_in, wo_in, mgain_ref, wid_ref, count_ref, sample_ref, out_ref,
    wq, wo, xp, normed, qkv, bias, hid, merged, recv, meta, msend,
    own_sem, ss, rs, a_send, a_recv, a_own, m_send, m_recv,
):
    pipe, tens = lax.axis_index("pipe"), lax.axis_index("tensor")
    y, c = pipe // CORES, pipe % CORES
    z, x = tens // CHIPS_X, tens % CHIPS_X
    weights = (wq, wo)
    features = x_ref.shape[1]
    blocks = x_ref.shape[0] // 128
    width = features // HEADS
    per_dest = 128 // group

    def slot(w, y_, z_, x_, half=None, core=c):
        rows = (wq_in, wo_in)[w].shape[0]
        start = (z_ * CHIPS_X + x_) * rows
        if half is not None:
            rows = rows // 2
            start = start + half * rows
        return weights[w].at[y_ * CORES + core, pl.ds(pl.multiple_of(start, 16), rows)]

    def copy(ref, send, receive, device):
        return pltpu.make_async_remote_copy(
            src_ref=ref, dst_ref=ref, send_sem=send, recv_sem=receive,
            device_id=device, device_id_type=MESH,
        )

    to_x = {"tensor": z * CHIPS_X + 1 - x}
    to_y = {"pipe": (1 - y) * CORES + c}
    to_core = {"pipe": y * CORES + 1 - c}
    to_up = {"tensor": (z + 1) * CHIPS_X + x}
    to_down = {"tensor": (z - 1) * CHIPS_X + x}

    def up(w, z_):
        return copy(slot(w, y, z_, x), ss.at[w, 0, z_], rs.at[w, 0, z_], to_up)

    def down(w, z_):
        return copy(slot(w, y, z_, x), ss.at[w, 1, z_], rs.at[w, 0, z_], to_down)

    names = ("x", "y", "xy", "yx", "c0", "cx", "cy", "cd")

    def other(w, z_, name):
        return {
            "x": lambda: copy(slot(w, y, z_, x), ss.at[w, 2, z_], rs.at[w, 1, z_], to_x),
            "y": lambda: copy(slot(w, y, z_, x), ss.at[w, 3, z_], rs.at[w, 2, z_], to_y),
            "xy": lambda: copy(slot(w, y, z_, 1 - x, 0), ss.at[w, 4, z_], rs.at[w, 3, z_], to_y),
            "yx": lambda: copy(slot(w, 1 - y, z_, x, 1), ss.at[w, 5, z_], rs.at[w, 4, z_], to_x),
            "c0": lambda: copy(slot(w, y, z_, x), ss.at[w, 6, z_], rs.at[w, 5, z_], to_core),
            "cx": lambda: copy(slot(w, y, z_, 1 - x), ss.at[w, 7, z_], rs.at[w, 6, z_], to_core),
            "cy": lambda: copy(slot(w, 1 - y, z_, x), ss.at[w, 8, z_], rs.at[w, 7, z_], to_core),
            "cd": lambda: copy(slot(w, 1 - y, z_, 1 - x), ss.at[w, 9, z_], rs.at[w, 8, z_], to_core),
        }[name]()

    def arrived(w, kind, z_, ref):
        copy(ref, ss.at[w, 0, z_], rs.at[w, kind, z_], to_x).wait_recv()

    def line_step(w, z_, own=False):
        if not own:
            arrived(w, 0, z_, slot(w, y, z_, x))

        @pl.when((z_ <= z) & (z < lines - 1))
        def _():
            up(w, z_).start()

        @pl.when((z_ >= z) & (z > 0))
        def _():
            down(w, z_).start()

        for name in ("x", "y", "c0"):
            other(w, z_, name).start()

    def plane_step(w, z_):
        arrived(w, 1, z_, slot(w, y, z_, 1 - x))
        other(w, z_, "xy").start()
        other(w, z_, "cx").start()
        arrived(w, 2, z_, slot(w, 1 - y, z_, x))
        other(w, z_, "yx").start()
        other(w, z_, "cy").start()

    def corner_step(w, z_):
        arrived(w, 3, z_, slot(w, 1 - y, z_, 1 - x, 0))
        arrived(w, 4, z_, slot(w, 1 - y, z_, 1 - x, 1))
        other(w, z_, "cd").start()

    offsets = [0]
    for far in range(1, lines):
        offsets += [-far, far]

    def when_valid(offset, fn, w):
        z_ = z + offset

        @pl.when((z_ >= 0) & (z_ < lines))
        def _():
            fn(w, z_)

    def gather_steps(w):
        steps = []
        for i in range(len(offsets) + 2):
            def step(i=i):
                if 0 < i < len(offsets):
                    when_valid(offsets[i], line_step, w)
                if 0 <= i - 1 < len(offsets):
                    when_valid(offsets[i - 1], plane_step, w)
                if 0 <= i - 2 < len(offsets):
                    when_valid(offsets[i - 2], corner_step, w)
            steps.append(step)
        return steps

    owns = [
        pltpu.make_async_copy(src, slot(w, y, z, x), own_sem.at[w])
        for w, src in enumerate((wq_in, wo_in))
    ]
    for own in owns:
        own.start()

    block_sample = []
    for block in range(blocks):
        offset = jnp.int32(0)
        value = jnp.int32(SAMPLES)
        for image in range(count_ref.shape[0]):
            units = count_ref[image] // 128
            inside = jnp.where(block >= offset, 1, 0) * jnp.where(block < offset + units, 1, 0)
            value = value + inside * (sample_ref[image] - SAMPLES)
            offset = offset + units
        block_sample.append(value)
    columns = group * blocks * per_dest
    lane_block = (lax.broadcasted_iota(jnp.int32, (8, columns), 1) // per_dest) % blocks
    own_meta = jnp.zeros((8, columns), jnp.int32)
    for block in range(blocks):
        own_meta = own_meta + jnp.where(lane_block == block, block_sample[block], 0)
    msend[...] = own_meta

    for w in (0, 1):
        owns[w].wait()
        line_step(w, z, own=True)

    to_row = lax.broadcasted_iota(jnp.int32, (128, 128), 0)
    from_row = lax.broadcasted_iota(jnp.int32, (128, 128), 1)
    source = (to_row % per_dest // 4) * (4 * group) + (to_row // per_dest) * 4 + to_row % 4
    permute = jnp.where(from_row == source, 1.0, 0.0).astype(jnp.bfloat16)
    wid = wid_ref[...].astype(jnp.float32).astype(jnp.bfloat16)
    across = (((1,), (1,)), ((), ()))
    wid_lane = lax.dot_general(wid, permute, across, preferred_element_type=jnp.float32)
    wid_row = lax.dot_general(permute, wid, across, preferred_element_type=jnp.float32)
    for block in range(blocks):
        same = wid_row[:, block : block + 1] == wid_lane[block : block + 1, :]
        bias[block] = jnp.where(same, 0.0, -1e30)

    def norm_block(block, carry):
        rows = pl.ds(pl.multiple_of(block * 128, 128), 128)
        moved = jnp.dot(permute, x_ref[rows, :], preferred_element_type=jnp.float32)
        xp[rows, :] = moved.astype(jnp.bfloat16)
        scale = lax.rsqrt(jnp.mean(moved * moved, axis=-1, keepdims=True) + epsilon)
        normed[rows, :] = (moved * scale * gain_ref[...]).astype(jnp.bfloat16)
        return carry

    lax.fori_loop(0, blocks, norm_block, 0)

    def meta_copy(m):
        peer = lax.rem(tens + m, group)
        return pltpu.make_async_remote_copy(
            src_ref=msend, dst_ref=meta.at[tens], send_sem=m_send.at[m - 1],
            recv_sem=m_recv.at[m - 1], device_id={"tensor": peer}, device_id_type=MESH,
        )

    for m in range(1, group):
        meta_copy(m).start()
    meta[tens] = own_meta

    for step in gather_steps(0):
        step()

    late = gather_steps(1)

    def core_arrived(w):
        for z_ in range(lines):
            arrived(w, 5, z_, slot(w, y, z_, x, core=1 - c))
            arrived(w, 6, z_, slot(w, y, z_, 1 - x, core=1 - c))
            arrived(w, 7, z_, slot(w, 1 - y, z_, x, core=1 - c))
            arrived(w, 8, z_, slot(w, 1 - y, z_, 1 - x, core=1 - c))

    core_arrived(0)
    part = wq_in.shape[1]
    for p in range(wq.shape[0]):
        for first in range(0, part, 256):
            last = min(first + 256, part)
            product = jnp.dot(
                normed[...], wq[p, :, first:last], preferred_element_type=jnp.float32
            )
            qkv[:, p * part + first : p * part + last] = product.astype(jnp.bfloat16)
            if late:
                late.pop(0)()
    while late:
        late.pop(0)()
    core_arrived(1)

    def exchange(block, m):
        peer = lax.rem(tens + m, group)
        return pltpu.make_async_remote_copy(
            src_ref=merged.at[block, pl.ds(pl.multiple_of(peer * per_dest, per_dest), per_dest)],
            dst_ref=recv.at[pl.ds(pl.multiple_of((tens * blocks + block) * per_dest, per_dest), per_dest)],
            send_sem=a_send.at[block, m - 1],
            recv_sem=a_recv.at[block, m - 1],
            device_id={"tensor": peer},
            device_id_type=MESH,
        )

    def keep(block):
        return pltpu.make_async_copy(
            merged.at[block, pl.ds(pl.multiple_of(tens * per_dest, per_dest), per_dest)],
            recv.at[pl.ds(pl.multiple_of((tens * blocks + block) * per_dest, per_dest), per_dest)],
            a_own.at[block],
        )

    out_part = wo_in.shape[1]

    def attend(block, carry):
        rows = pl.ds(pl.multiple_of(block * 128, 128), 128)
        pieces = [None] * (features // 128)
        mask = bias[block]
        for head in range(HEADS):
            low, high = head * width, (head + 1) * width
            g0, g1 = low // 128, (high - 1) // 128 + 1
            lanes = lax.broadcasted_iota(jnp.int32, (128, (g1 - g0) * 128), 1) + g0 * 128
            in_head = (lanes >= low) & (lanes < high)
            query = qkv[rows, g0 * 128 : g1 * 128]
            key = qkv[rows, features + g0 * 128 : features + g1 * 128]
            value = qkv[rows, 2 * features + g0 * 128 : 2 * features + g1 * 128]
            query = jnp.where(in_head, query, jnp.zeros_like(query))
            score = lax.dot_general(query, key, across, preferred_element_type=jnp.float32)
            score = score * (1.0 / math.sqrt(width)) + mask
            weight = jnp.exp(score - jnp.max(score, axis=-1, keepdims=True))
            total = jnp.sum(weight, axis=-1, keepdims=True)
            mixed = jnp.dot(
                weight.astype(jnp.bfloat16), value, preferred_element_type=jnp.float32
            ) * (1.0 / total)
            for g in range(g0, g1):
                cut = slice((g - g0) * 128, (g - g0 + 1) * 128)
                piece = mixed[:, cut]
                if pieces[g] is not None:
                    piece = jnp.where(in_head[:, cut], piece, pieces[g])
                pieces[g] = piece
        live = jnp.float32(0)
        for other in range(blocks):
            alive = jnp.where(block_sample[other] < SAMPLES, 1.0, 0.0)
            live = live + jnp.where(block == other, alive, 0.0)
        context = (jnp.concatenate(pieces, axis=1) * live).astype(jnp.bfloat16)
        for p in range(wo.shape[0]):
            hid[:, p * out_part : (p + 1) * out_part] = jnp.dot(
                context, wo[p], preferred_element_type=jnp.float32
            )
        hidden = hid[...] + xp[rows, :].astype(jnp.float32)
        scale = lax.rsqrt(jnp.mean(hidden * hidden, axis=-1, keepdims=True) + epsilon)
        merged[block] = (hidden * scale * mgain_ref[...]).astype(jnp.bfloat16)
        for m in range(1, group):
            exchange(block, m).start()
        keep(block).start()
        return carry

    lax.fori_loop(0, blocks, attend, 0)

    for m in range(1, group):
        meta_copy(m).wait()
    lane = lax.broadcasted_iota(jnp.int32, (1, columns), 1)
    sample_lane = jnp.zeros((1, columns), jnp.int32)
    for source_rank in range(group):
        sample_lane = sample_lane + jnp.where(
            lane // (blocks * per_dest) == source_rank, meta[source_rank, 0:1, :], 0
        )
    order = (sample_lane * columns + lane).astype(jnp.float32)
    order_down = jnp.transpose(jnp.broadcast_to(order, (128, columns)))
    ranks = []
    for first in range(0, columns, 128):
        before = jnp.where(order_down < order[:, first : first + 128], 1.0, 0.0)
        ranks.append(jnp.sum(before, axis=0, keepdims=True))
    rank = jnp.concatenate(ranks, axis=1)
    rank = jnp.where(sample_lane < SAMPLES, rank, -1.0)

    def drain(block, carry):
        for m in range(1, group):
            exchange(block, m).wait()
        keep(block).wait()
        return carry

    lax.fori_loop(0, blocks, drain, 0)

    tokens = out_ref.shape[0]
    target = (lax.broadcasted_iota(jnp.int32, (tokens, columns), 0) * 4).astype(jnp.float32)
    for k in range(4):
        place = jnp.where(rank == target + k, 1.0, 0.0).astype(jnp.bfloat16)
        placed = jnp.dot(place, recv[...], preferred_element_type=jnp.float32)
        out_ref[:, k * features : (k + 1) * features] = placed.astype(jnp.bfloat16)

    for w in (0, 1):
        for z_ in range(lines):
            for name in names:
                other(w, z_, name).wait_send()

            @pl.when((z_ <= z) & (z < lines - 1))
            def _():
                up(w, z_).wait_send()

            @pl.when((z_ >= z) & (z > 0))
            def _():
                down(w, z_).wait_send()


def fused_body(pipe, group, patches, attn_gain, w_qkv, w_out, merge_gain, window_ids, image_patches, image_sample):
    slots, features = patches.shape
    blocks = slots // 128
    lines = group // CHIPS_X
    columns = group * blocks * (128 // group)
    bf16, f32, i32 = jnp.bfloat16, jnp.float32, jnp.int32
    vmem = pl.BlockSpec(memory_space=pltpu.VMEM)
    smem = pl.BlockSpec(memory_space=pltpu.SMEM)
    hbm = pl.BlockSpec(memory_space=pl.ANY)
    dma = pltpu.SemaphoreType.DMA
    placed = pl.pallas_call(
        functools.partial(kernel, lines, group),
        out_shape=jax.ShapeDtypeStruct((slots // 4, 4 * features), bf16),
        in_specs=[vmem, vmem, hbm, hbm, vmem, vmem, smem, smem],
        out_specs=vmem,
        scratch_shapes=[
            pltpu.VMEM((pipe, w_qkv.shape[0] * group, w_qkv.shape[1]), bf16),
            pltpu.VMEM((pipe, w_out.shape[0] * group, w_out.shape[1]), bf16),
            pltpu.VMEM((slots, features), bf16),
            pltpu.VMEM((slots, features), bf16),
            pltpu.VMEM((slots, 3 * features), bf16),
            pltpu.VMEM((blocks, 128, 128), f32),
            pltpu.VMEM((128, features), f32),
            pltpu.VMEM((blocks, 128, features), bf16),
            pltpu.VMEM((slots, features), bf16),
            pltpu.VMEM((group, 8, columns), i32),
            pltpu.VMEM((8, columns), i32),
            dma((2,)),
            dma((2, 10, lines)),
            dma((2, 9, lines)),
            dma((blocks, group - 1)),
            dma((blocks, group - 1)),
            dma((blocks,)),
            dma((group - 1,)),
            dma((group - 1,)),
        ],
        compiler_params=pltpu.CompilerParams(
            has_side_effects=True, vmem_limit_bytes=60 * 1024 * 1024
        ),
    )(
        patches, attn_gain[None, :], w_qkv, w_out, merge_gain[None, :],
        window_ids.reshape(blocks, 128), image_patches, image_sample,
    )
    return placed.reshape(1, slots // 4, 1, 4 * features)


def fits(mesh):
    return mesh.shape["pipe"] == 2 * CORES and mesh.shape["tensor"] == 8


def solution(mesh):
    chosen = body
    if fits(mesh):
        chosen = functools.partial(fused_body, mesh.shape["pipe"], mesh.shape["tensor"])
    return jax.shard_map(
        chosen,
        mesh=mesh,
        in_specs=(
            P(("pipe", "tensor"), None),
            P(),
            P("tensor", "pipe"),
            P("tensor", "pipe"),
            P(),
            P(("pipe", "tensor")),
            P(("pipe", "tensor")),
            P(("pipe", "tensor")),
        ),
        out_specs=P("pipe", None, "tensor", None),
        check_vma=False,
    )
```

```python
import functools
import math

import jax
import jax.numpy as jnp
from jax import lax
from jax.experimental import pallas as pl
from jax.experimental.pallas import tpu as pltpu
from jax.sharding import PartitionSpec as P

HEADS = 16
WINDOW = 64
SAMPLES = 8


epsilon = 1e-06


def normalize(values, gain_row):
    return (
        values * lax.rsqrt(jnp.mean(values * values, axis=-1, keepdims=True) + epsilon) * gain_row
    )


def token_positions(starts, merged_count, token_count):
    offsets = jnp.cumsum(merged_count) - merged_count
    token_index = jnp.arange(token_count, dtype=jnp.int32)
    inside = (token_index[None, :] >= offsets[:, None]) & (
        token_index[None, :] < (offsets + merged_count)[:, None]
    )
    position = jnp.sum(
        jnp.where(inside, starts[:, None] + token_index[None, :] - offsets[:, None], 0), axis=0
    )
    return jnp.where(jnp.any(inside, axis=0), position, -1)


def body(patches, attn_gain, w_qkv, w_out, merge_gain, window_ids, image_patches, image_sample):
    patch_count, feature_width = patches.shape
    token_count = patch_count // 4
    group_size = lax.axis_size("tensor")
    own_index = lax.axis_index("tensor")
    residual = patches.astype(jnp.float32)
    normed = normalize(residual, attn_gain).astype(jnp.bfloat16)
    qkv_rows = lax.all_gather(w_qkv, "tensor", axis=0, tiled=True)
    qkv = jnp.dot(
        normed,
        lax.all_gather(qkv_rows, "pipe", axis=1, tiled=True),
        preferred_element_type=jnp.float32,
    ).astype(jnp.bfloat16)
    head_width = feature_width // HEADS
    tile_count = patch_count // WINDOW

    def split_heads(block):
        return block.reshape(tile_count, WINDOW, HEADS, head_width)

    queries = split_heads(qkv[:, :feature_width])
    keys_tile = split_heads(qkv[:, feature_width : 2 * feature_width])
    values_tile = split_heads(qkv[:, 2 * feature_width :])
    scores = jnp.einsum(
        "tqhd,tkhd->thqk", queries, keys_tile, preferred_element_type=jnp.float32
    ) * (1.0 / math.sqrt(head_width))
    live_row = jnp.arange(patch_count, dtype=jnp.int32) < jnp.sum(image_patches)
    window_tile = window_ids.reshape(tile_count, WINDOW)
    live_tile = live_row.reshape(tile_count, WINDOW)
    allowed = (window_tile[:, :, None] == window_tile[:, None, :]) & live_tile[:, None, :]
    scores = jnp.where(allowed[:, None, :, :], scores, -1e30)
    row_max = jnp.max(scores, axis=-1, keepdims=True)
    exponent = jnp.exp(scores - row_max)
    weights = (exponent / jnp.sum(exponent, axis=-1, keepdims=True)).astype(jnp.bfloat16)
    context = jnp.einsum(
        "thqk,tkhd->tqhd", weights, values_tile, preferred_element_type=jnp.float32
    ).reshape(patch_count, feature_width)
    context = jnp.where(live_row[:, None], context, 0.0).astype(jnp.bfloat16)
    proj_rows = lax.all_gather(w_out, "tensor", axis=0, tiled=True)
    attended = jnp.dot(
        context,
        lax.all_gather(proj_rows, "pipe", axis=1, tiled=True),
        preferred_element_type=jnp.float32,
    )
    hidden = residual + attended
    merged = (
        normalize(hidden, merge_gain).astype(jnp.bfloat16).reshape(token_count, 4 * feature_width)
    )
    outgoing = merged.reshape(token_count // group_size, group_size, 4 * feature_width)
    merged_count = image_patches // 4
    sample_hot = image_sample[:, None] == jnp.arange(SAMPLES, dtype=jnp.int32)[None, :]
    sample_tally = jnp.sum(jnp.where(sample_hot, merged_count[:, None], 0), axis=0)
    all_tallies = lax.all_gather(sample_tally[None, :], "tensor", axis=0, tiled=True)
    source_ranks = jnp.arange(group_size, dtype=jnp.int32)
    before = jnp.sum(jnp.where((source_ranks < own_index)[:, None], all_tallies, 0), axis=0)
    totals = jnp.sum(all_tallies, axis=0)
    sample_index = jnp.arange(SAMPLES, dtype=jnp.int32)
    sample_base = jnp.sum(
        jnp.where(sample_index[None, :] < sample_index[:, None], totals[None, :], 0), axis=1
    )
    image_order = jnp.arange(image_sample.shape[0], dtype=jnp.int32)
    same_before = (image_sample[None, :] == image_sample[:, None]) & (
        image_order[None, :] < image_order[:, None]
    )
    earlier = jnp.sum(jnp.where(same_before, merged_count[None, :], 0), axis=1)
    starts = jnp.sum(jnp.where(sample_hot, (sample_base + before)[None, :], 0), axis=1) + earlier
    position = token_positions(starts, merged_count, token_count)
    outgoing_position = position.reshape(token_count // group_size, group_size)
    received, received_position = (
        lax.all_to_all(outgoing, "tensor", split_axis=1, concat_axis=0, tiled=True),
        lax.all_to_all(outgoing_position, "tensor", split_axis=1, concat_axis=0, tiled=True),
    )
    dest_rows = received_position.reshape(token_count) // group_size
    placement = (jnp.arange(token_count, dtype=jnp.int32)[:, None] == dest_rows[None, :]).astype(
        jnp.bfloat16
    )
    placed = jnp.dot(
        placement,
        received.reshape(token_count, 4 * feature_width),
        preferred_element_type=jnp.float32,
    )
    return placed.astype(jnp.bfloat16).reshape(1, token_count, 1, 4 * feature_width)


CORES = 2
CHIPS_X = 2
MESH = pl.DeviceIdType.MESH


def kernel(
    lines, group, x_ref, gain_ref, wq_in, wo_in, mgain_ref, wid_ref, count_ref, sample_ref, out_ref,
    wq, wo, xp, normed, qkv, context, bias, hid, merged, recv, meta, msend,
    own_sem, ss, rs, a_send, a_recv, a_own, m_send, m_recv,
):
    pipe, tens = lax.axis_index("pipe"), lax.axis_index("tensor")
    y, c = pipe // CORES, pipe % CORES
    z, x = tens // CHIPS_X, tens % CHIPS_X
    weights = (wq, wo)
    features = x_ref.shape[1]
    blocks = x_ref.shape[0] // 128
    width = features // HEADS
    per_dest = 128 // group

    def slot(w, y_, z_, x_, half=None, core=c):
        rows = (wq_in, wo_in)[w].shape[0]
        start = (z_ * CHIPS_X + x_) * rows
        if half is not None:
            rows = rows // 2
            start = start + half * rows
        return weights[w].at[y_ * CORES + core, pl.ds(pl.multiple_of(start, 16), rows)]

    def copy(ref, send, receive, device):
        return pltpu.make_async_remote_copy(
            src_ref=ref, dst_ref=ref, send_sem=send, recv_sem=receive,
            device_id=device, device_id_type=MESH,
        )

    to_x = {"tensor": z * CHIPS_X + 1 - x}
    to_y = {"pipe": (1 - y) * CORES + c}
    to_core = {"pipe": y * CORES + 1 - c}
    to_up = {"tensor": (z + 1) * CHIPS_X + x}
    to_down = {"tensor": (z - 1) * CHIPS_X + x}

    def up(w, z_):
        return copy(slot(w, y, z_, x), ss.at[w, 0, z_], rs.at[w, 0, z_], to_up)

    def down(w, z_):
        return copy(slot(w, y, z_, x), ss.at[w, 1, z_], rs.at[w, 0, z_], to_down)

    names = ("x", "y", "xy", "yx", "c0", "cx", "cy", "cd")

    def other(w, z_, name):
        return {
            "x": lambda: copy(slot(w, y, z_, x), ss.at[w, 2, z_], rs.at[w, 1, z_], to_x),
            "y": lambda: copy(slot(w, y, z_, x), ss.at[w, 3, z_], rs.at[w, 2, z_], to_y),
            "xy": lambda: copy(slot(w, y, z_, 1 - x, 0), ss.at[w, 4, z_], rs.at[w, 3, z_], to_y),
            "yx": lambda: copy(slot(w, 1 - y, z_, x, 1), ss.at[w, 5, z_], rs.at[w, 4, z_], to_x),
            "c0": lambda: copy(slot(w, y, z_, x), ss.at[w, 6, z_], rs.at[w, 5, z_], to_core),
            "cx": lambda: copy(slot(w, y, z_, 1 - x), ss.at[w, 7, z_], rs.at[w, 6, z_], to_core),
            "cy": lambda: copy(slot(w, 1 - y, z_, x), ss.at[w, 8, z_], rs.at[w, 7, z_], to_core),
            "cd": lambda: copy(slot(w, 1 - y, z_, 1 - x), ss.at[w, 9, z_], rs.at[w, 8, z_], to_core),
        }[name]()

    def arrived(w, kind, z_, ref):
        copy(ref, ss.at[w, 0, z_], rs.at[w, kind, z_], to_x).wait_recv()

    def line_step(w, z_, own=False):
        if not own:
            arrived(w, 0, z_, slot(w, y, z_, x))

        @pl.when((z_ <= z) & (z < lines - 1))
        def _():
            up(w, z_).start()

        @pl.when((z_ >= z) & (z > 0))
        def _():
            down(w, z_).start()

        for name in ("x", "y", "c0"):
            other(w, z_, name).start()

    def plane_step(w, z_):
        arrived(w, 1, z_, slot(w, y, z_, 1 - x))
        other(w, z_, "xy").start()
        other(w, z_, "cx").start()
        arrived(w, 2, z_, slot(w, 1 - y, z_, x))
        other(w, z_, "yx").start()
        other(w, z_, "cy").start()

    def corner_step(w, z_):
        arrived(w, 3, z_, slot(w, 1 - y, z_, 1 - x, 0))
        arrived(w, 4, z_, slot(w, 1 - y, z_, 1 - x, 1))
        other(w, z_, "cd").start()

    offsets = [0]
    for far in range(1, lines):
        offsets += [-far, far]

    def when_valid(offset, fn, w):
        z_ = z + offset

        @pl.when((z_ >= 0) & (z_ < lines))
        def _():
            fn(w, z_)

    owns = [
        pltpu.make_async_copy(src, slot(w, y, z, x), own_sem.at[w])
        for w, src in enumerate((wq_in, wo_in))
    ]
    for own in owns:
        own.start()

    block_sample = []
    for block in range(blocks):
        offset = jnp.int32(0)
        value = jnp.int32(SAMPLES)
        for image in range(count_ref.shape[0]):
            units = count_ref[image] // 128
            inside = jnp.where(block >= offset, 1, 0) * jnp.where(block < offset + units, 1, 0)
            value = value + inside * (sample_ref[image] - SAMPLES)
            offset = offset + units
        block_sample.append(value)
    columns = group * blocks * per_dest
    lane_block = (lax.broadcasted_iota(jnp.int32, (8, columns), 1) // per_dest) % blocks
    own_meta = jnp.zeros((8, columns), jnp.int32)
    for block in range(blocks):
        own_meta = own_meta + jnp.where(lane_block == block, block_sample[block], 0)
    msend[...] = own_meta

    for w in (0, 1):
        owns[w].wait()
        line_step(w, z, own=True)

    to_row = lax.broadcasted_iota(jnp.int32, (128, 128), 0)
    from_row = lax.broadcasted_iota(jnp.int32, (128, 128), 1)
    source = (to_row % per_dest // 4) * (4 * group) + (to_row // per_dest) * 4 + to_row % 4
    permute = jnp.where(from_row == source, 1.0, 0.0).astype(jnp.bfloat16)
    wid = wid_ref[...].astype(jnp.float32).astype(jnp.bfloat16)
    across = (((1,), (1,)), ((), ()))
    wid_lane = lax.dot_general(wid, permute, across, preferred_element_type=jnp.float32)
    wid_row = lax.dot_general(permute, wid, across, preferred_element_type=jnp.float32)
    for block in range(blocks):
        same = wid_row[:, block : block + 1] == wid_lane[block : block + 1, :]
        bias[block] = jnp.where(same, 0.0, -1e30)

    def norm_block(block, carry):
        rows = pl.ds(pl.multiple_of(block * 128, 128), 128)
        moved = jnp.dot(permute, x_ref[rows, :], preferred_element_type=jnp.float32)
        xp[rows, :] = moved.astype(jnp.bfloat16)
        scale = lax.rsqrt(jnp.mean(moved * moved, axis=-1, keepdims=True) + epsilon)
        normed[rows, :] = (moved * scale * gain_ref[...]).astype(jnp.bfloat16)
        return carry

    lax.fori_loop(0, blocks, norm_block, 0)

    def meta_copy(m):
        peer = lax.rem(tens + m, group)
        return pltpu.make_async_remote_copy(
            src_ref=msend, dst_ref=meta.at[tens], send_sem=m_send.at[m - 1],
            recv_sem=m_recv.at[m - 1], device_id={"tensor": peer}, device_id_type=MESH,
        )

    for m in range(1, group):
        meta_copy(m).start()
    meta[tens] = own_meta

    lag = 3
    for i in range(len(offsets) + lag):
        if 0 < i < len(offsets):
            when_valid(offsets[i], line_step, 0)
        if i >= lag:
            when_valid(offsets[i - lag], plane_step, 0)
    for offset in offsets[1:]:
        when_valid(offset, line_step, 1)

    def core_arrived(w, own_plane):
        for z_ in range(lines):
            if own_plane:
                arrived(w, 5, z_, slot(w, y, z_, x, core=1 - c))
                arrived(w, 6, z_, slot(w, y, z_, 1 - x, core=1 - c))
            else:
                arrived(w, 7, z_, slot(w, 1 - y, z_, x, core=1 - c))
                arrived(w, 8, z_, slot(w, 1 - y, z_, 1 - x, core=1 - c))

    part = wq_in.shape[1]

    def project(plane, between):
        for core in range(CORES):
            for first in range(0, part, 256):
                last = min(first + 256, part)
                product = jnp.dot(
                    normed[...],
                    wq[plane * CORES + core, :, first:last],
                    preferred_element_type=jnp.float32,
                )
                qkv[plane, :, core * part + first : core * part + last] = product.astype(jnp.bfloat16)
                if between:
                    between.pop(0)()

    core_arrived(0, True)
    project(y, [])
    for offset in offsets:
        when_valid(offset, corner_step, 0)
    core_arrived(0, False)
    project(
        1 - y, [functools.partial(when_valid, offset, plane_step, 1) for offset in offsets]
    )

    def exchange(block, m):
        peer = lax.rem(tens + m, group)
        return pltpu.make_async_remote_copy(
            src_ref=merged.at[block, pl.ds(pl.multiple_of(peer * per_dest, per_dest), per_dest)],
            dst_ref=recv.at[pl.ds(pl.multiple_of((tens * blocks + block) * per_dest, per_dest), per_dest)],
            send_sem=a_send.at[block, m - 1],
            recv_sem=a_recv.at[block, m - 1],
            device_id={"tensor": peer},
            device_id_type=MESH,
        )

    def keep(block):
        return pltpu.make_async_copy(
            merged.at[block, pl.ds(pl.multiple_of(tens * per_dest, per_dest), per_dest)],
            recv.at[pl.ds(pl.multiple_of((tens * blocks + block) * per_dest, per_dest), per_dest)],
            a_own.at[block],
        )

    out_part = wo_in.shape[1]
    ahead = min(2, blocks)

    half = qkv.shape[2]

    def lanes_of(rows, start, stop):
        plane = start // half
        return qkv[plane, rows, start - plane * half : stop - plane * half]

    def attend(block, carry):
        rows = pl.ds(pl.multiple_of(block * 128, 128), 128)
        pieces = [None] * (features // 128)
        mask = bias[block]
        for head in range(HEADS):
            low, high = head * width, (head + 1) * width
            g0, g1 = low // 128, (high - 1) // 128 + 1
            lanes = lax.broadcasted_iota(jnp.int32, (128, (g1 - g0) * 128), 1) + g0 * 128
            in_head = (lanes >= low) & (lanes < high)
            query, key, value = (
                lanes_of(rows, i * features + g0 * 128, i * features + g1 * 128) for i in range(3)
            )
            query = jnp.where(in_head, query, jnp.zeros_like(query))
            score = lax.dot_general(query, key, across, preferred_element_type=jnp.float32)
            score = score * (1.0 / math.sqrt(width)) + mask
            weight = jnp.exp(score - jnp.max(score, axis=-1, keepdims=True))
            total = jnp.sum(weight, axis=-1, keepdims=True)
            mixed = jnp.dot(
                weight.astype(jnp.bfloat16), value, preferred_element_type=jnp.float32
            ) * (1.0 / total)
            for g in range(g0, g1):
                cut = slice((g - g0) * 128, (g - g0 + 1) * 128)
                piece = mixed[:, cut]
                if pieces[g] is not None:
                    piece = jnp.where(in_head[:, cut], piece, pieces[g])
                pieces[g] = piece
        live = jnp.float32(0)
        for other_block in range(blocks):
            alive = jnp.where(block_sample[other_block] < SAMPLES, 1.0, 0.0)
            live = live + jnp.where(block == other_block, alive, 0.0)
        for g, piece in enumerate(pieces):
            context[rows, g * 128 : (g + 1) * 128] = (piece * live).astype(jnp.bfloat16)
        return carry

    def finish(block, carry):
        rows = pl.ds(pl.multiple_of(block * 128, 128), 128)
        for p in range(wo.shape[0]):
            hid[:, p * out_part : (p + 1) * out_part] = jnp.dot(
                context[rows, :], wo[p], preferred_element_type=jnp.float32
            )
        hidden = hid[...] + xp[rows, :].astype(jnp.float32)
        scale = lax.rsqrt(jnp.mean(hidden * hidden, axis=-1, keepdims=True) + epsilon)
        merged[block] = (hidden * scale * mgain_ref[...]).astype(jnp.bfloat16)
        for m in range(1, group):
            exchange(block, m).start()
        keep(block).start()
        return carry

    lax.fori_loop(0, ahead, attend, 0)
    for offset in offsets:
        when_valid(offset, corner_step, 1)
    core_arrived(1, True)
    core_arrived(1, False)

    def pair(block, carry):
        finish(block, carry)

        @pl.when(block + ahead < blocks)
        def _():
            attend(block + ahead, 0)

        return carry

    lax.fori_loop(0, blocks, pair, 0)

    for m in range(1, group):
        meta_copy(m).wait()
    lane = lax.broadcasted_iota(jnp.int32, (1, columns), 1)
    sample_lane = jnp.zeros((1, columns), jnp.int32)
    for source_rank in range(group):
        sample_lane = sample_lane + jnp.where(
            lane // (blocks * per_dest) == source_rank, meta[source_rank, 0:1, :], 0
        )
    order = (sample_lane * columns + lane).astype(jnp.float32)
    order_down = jnp.transpose(jnp.broadcast_to(order, (128, columns)))
    ranks = []
    for first in range(0, columns, 128):
        before = jnp.where(order_down < order[:, first : first + 128], 1.0, 0.0)
        ranks.append(jnp.sum(before, axis=0, keepdims=True))
    rank = jnp.concatenate(ranks, axis=1)
    rank = jnp.where(sample_lane < SAMPLES, rank, -1.0)

    def drain(block, carry):
        for m in range(1, group):
            exchange(block, m).wait()
        keep(block).wait()
        return carry

    lax.fori_loop(0, blocks, drain, 0)

    tokens = out_ref.shape[0]
    target = (lax.broadcasted_iota(jnp.int32, (tokens, columns), 0) * 4).astype(jnp.float32)
    for k in range(4):
        place = jnp.where(rank == target + k, 1.0, 0.0).astype(jnp.bfloat16)
        placed = jnp.dot(place, recv[...], preferred_element_type=jnp.float32)
        out_ref[:, k * features : (k + 1) * features] = placed.astype(jnp.bfloat16)

    for w in (0, 1):
        for z_ in range(lines):
            for name in names:
                other(w, z_, name).wait_send()

            @pl.when((z_ <= z) & (z < lines - 1))
            def _():
                up(w, z_).wait_send()

            @pl.when((z_ >= z) & (z > 0))
            def _():
                down(w, z_).wait_send()


def fused_body(pipe, group, patches, attn_gain, w_qkv, w_out, merge_gain, window_ids, image_patches, image_sample):
    slots, features = patches.shape
    blocks = slots // 128
    lines = group // CHIPS_X
    columns = group * blocks * (128 // group)
    bf16, f32, i32 = jnp.bfloat16, jnp.float32, jnp.int32
    vmem = pl.BlockSpec(memory_space=pltpu.VMEM)
    smem = pl.BlockSpec(memory_space=pltpu.SMEM)
    hbm = pl.BlockSpec(memory_space=pl.ANY)
    dma = pltpu.SemaphoreType.DMA
    placed = pl.pallas_call(
        functools.partial(kernel, lines, group),
        out_shape=jax.ShapeDtypeStruct((slots // 4, 4 * features), bf16),
        in_specs=[vmem, vmem, hbm, hbm, vmem, vmem, smem, smem],
        out_specs=vmem,
        scratch_shapes=[
            pltpu.VMEM((pipe, w_qkv.shape[0] * group, w_qkv.shape[1]), bf16),
            pltpu.VMEM((pipe, w_out.shape[0] * group, w_out.shape[1]), bf16),
            pltpu.VMEM((slots, features), bf16),
            pltpu.VMEM((slots, features), bf16),
            pltpu.VMEM((pipe // CORES, slots, CORES * w_qkv.shape[1]), bf16),
            pltpu.VMEM((slots, features), bf16),
            pltpu.VMEM((blocks, 128, 128), f32),
            pltpu.VMEM((128, features), f32),
            pltpu.VMEM((blocks, 128, features), bf16),
            pltpu.VMEM((slots, features), bf16),
            pltpu.VMEM((group, 8, columns), i32),
            pltpu.VMEM((8, columns), i32),
            dma((2,)),
            dma((2, 10, lines)),
            dma((2, 9, lines)),
            dma((blocks, group - 1)),
            dma((blocks, group - 1)),
            dma((blocks,)),
            dma((group - 1,)),
            dma((group - 1,)),
        ],
        compiler_params=pltpu.CompilerParams(
            has_side_effects=True, vmem_limit_bytes=60 * 1024 * 1024
        ),
    )(
        patches, attn_gain[None, :], w_qkv, w_out, merge_gain[None, :],
        window_ids.reshape(blocks, 128), image_patches, image_sample,
    )
    return placed.reshape(1, slots // 4, 1, 4 * features)


def fits(mesh):
    return mesh.shape["pipe"] == 2 * CORES and mesh.shape["tensor"] == 8


def solution(mesh):
    chosen = body
    if fits(mesh):
        chosen = functools.partial(fused_body, mesh.shape["pipe"], mesh.shape["tensor"])
    return jax.shard_map(
        chosen,
        mesh=mesh,
        in_specs=(
            P(("pipe", "tensor"), None),
            P(),
            P("tensor", "pipe"),
            P("tensor", "pipe"),
            P(),
            P(("pipe", "tensor")),
            P(("pipe", "tensor")),
            P(("pipe", "tensor")),
        ),
        out_specs=P("pipe", None, "tensor", None),
        check_vma=False,
    )
```
